32 devices in a mesh: dp: 1 (over z), tp: 32 (over y, x, core).
Axes of the slice: x: 4, y: 4, z: 1, core: 2. Of those that a mesh axis runs over, the one named last changes fastest.
The devices are a block of a 4x4x8 slice.
Arguments:
- hidden: bfloat16 [8192, 1024], P(('dp', 'tp'))
- w_two: bfloat16 [1024, 1024], replicated
- ln_scale: float32 [2, 1024], replicated
- ln_shift: float32 [2, 1024], replicated
- embed: bfloat16 [53248, 1024], P('tp')
- targets: int32 [2, 8192], P(None, ('dp', 'tp'))
- loss_mask: int32 [2, 8192], P(None, ('dp', 'tp'))
Outputs:
- output 1: float32 [2, 8192], P(None, ('dp', 'tp'))
- output 2: float32 [1], P('dp')
- output 3: bfloat16 [8192, 1024], P(('dp', 'tp'))
- output 4: float32 [53248, 1024], P(('dp', 'tp'))
- output 5: float32 [1024, 1024], P('dp')
- output 6: float32 [2, 1024], P('dp')
- output 7: float32 [2, 1024], P('dp')
All inputs are finite; a program needn't handle non-finite values.
Results may differ from the reference program's by a relative error of at most 0.00599148.
Values are sent between devices in bfloat16 or wider.
A program may use at most 768 MiB of HBM per device.

```python
import math
import jax
import jax.numpy as jnp
from jax import lax

TOKENS_DEV = 256
GROUP_SIZE = 32
D_MODEL = 1024
VOCAB_SIZE = 50257
TABLE_ROWS = 53248

TOKENS = TOKENS_DEV * GROUP_SIZE
ROW_BLOCK = math.gcd(TOKENS, 128)
BLOCKS = TOKENS // ROW_BLOCK
LN_EPS = 1e-5


def setup_inputs(seed: int = 0, part: int = 0) -> dict:
    base = jax.random.key(seed)
    k_w, k_g, k_b, k_e = jax.random.split(base, 4)
    part_key = jax.random.fold_in(base, part)
    k_h, k_t, k_m, k_l = jax.random.split(part_key, 4)
    hidden = jax.random.normal(k_h, (TOKENS, D_MODEL), jnp.float32).astype(jnp.bfloat16)
    w_two = (jax.random.normal(k_w, (D_MODEL, D_MODEL), jnp.float32) * D_MODEL ** -0.5).astype(jnp.bfloat16)
    ln_scale = 1.0 + 0.3 * jax.random.normal(k_g, (2, D_MODEL), jnp.float32)
    ln_shift = 0.3 * jax.random.normal(k_b, (2, D_MODEL), jnp.float32)
    embed = (jax.random.normal(k_e, (TABLE_ROWS, D_MODEL), jnp.float32) * (2.5 * D_MODEL ** -0.5)).astype(jnp.bfloat16)
    targets = jax.random.randint(k_t, (2, TOKENS), 0, VOCAB_SIZE, jnp.int32)
    keep_len = jax.random.randint(k_l, (2, GROUP_SIZE, 1), TOKENS_DEV // 4, TOKENS_DEV + 1, jnp.int32)
    keep_draw = jax.random.randint(k_m, (2, GROUP_SIZE, TOKENS_DEV), 0, 8, jnp.int32)
    position = jnp.arange(TOKENS_DEV, dtype=jnp.int32)
    keep = (position < keep_len) & ((keep_draw != 0) | (position == 0))
    loss_mask = keep.astype(jnp.int32).reshape(2, TOKENS)
    return {'hidden': hidden, 'w_two': w_two, 'ln_scale': ln_scale, 'ln_shift': ln_shift,
            'embed': embed, 'targets': targets, 'loss_mask': loss_mask}


def layer_norm(values, gain, bias):
    mean_val = jnp.mean(values, axis=-1, keepdims=True)
    centered = values - mean_val
    variance = jnp.mean(centered * centered, axis=-1, keepdims=True)
    return centered * lax.rsqrt(variance + LN_EPS) * gain + bias


def reference(hidden, w_two, ln_scale, ln_shift, embed, targets, loss_mask):
    proj_out = jnp.dot(hidden, w_two, preferred_element_type=jnp.float32).astype(jnp.bfloat16)
    norm_input = jnp.stack([hidden.astype(jnp.float32), proj_out.astype(jnp.float32)])
    normed, ln_back = jax.vjp(jax.vmap(layer_norm), norm_input, ln_scale, ln_shift)
    x_both = normed.astype(jnp.bfloat16)
    mask_f = loss_mask.astype(jnp.float32)
    token_count = jnp.sum(mask_f, axis=1)
    weight = mask_f / token_count[:, None]
    x_blocks = jnp.swapaxes(x_both.reshape(2, BLOCKS, ROW_BLOCK, D_MODEL), 0, 1)
    t_blocks = jnp.swapaxes(targets.reshape(2, BLOCKS, ROW_BLOCK), 0, 1)
    w_blocks = jnp.swapaxes(weight.reshape(2, BLOCKS, ROW_BLOCK), 0, 1)
    col_ids = jnp.arange(TABLE_ROWS, dtype=jnp.int32)

    def block_step(d_embed, block):
        x_blk, t_blk, w_blk = block
        raw_rows = []
        dx_rows = []
        for head_idx in range(2):
            logits = jnp.dot(x_blk[head_idx], embed.T, preferred_element_type=jnp.float32)
            log_norm = jax.nn.logsumexp(logits, axis=-1)
            is_target = col_ids[None, :] == t_blk[head_idx][:, None]
            tgt_logit = jnp.sum(jnp.where(is_target, logits, 0.0), axis=-1)
            probs_val = jnp.exp(logits - log_norm[:, None])
            d_logits = ((probs_val - is_target.astype(jnp.float32)) * w_blk[head_idx][:, None]).astype(jnp.bfloat16)
            d_embed = d_embed + jnp.dot(d_logits.T, x_blk[head_idx], preferred_element_type=jnp.float32)
            dx_rows.append(jnp.dot(d_logits, embed, preferred_element_type=jnp.float32))
            raw_rows.append(log_norm - tgt_logit)
        return d_embed, (jnp.stack(raw_rows), jnp.stack(dx_rows))

    d_embed, (raw_loss, d_x) = lax.scan(block_step, jnp.zeros((TABLE_ROWS, D_MODEL), jnp.float32),
                                        (x_blocks, t_blocks, w_blocks))
    raw_loss = jnp.swapaxes(raw_loss, 0, 1).reshape(2, TOKENS)
    d_x = jnp.swapaxes(d_x, 0, 1).reshape(2, TOKENS, D_MODEL)
    token_loss = raw_loss * mask_f
    total_loss = jnp.sum(token_loss / token_count[:, None]).reshape(1)
    d_norm_in, d_ln_scale, d_ln_shift = ln_back(d_x)
    d_proj = d_norm_in[1].astype(jnp.bfloat16)
    d_hidden = (d_norm_in[0] + jnp.dot(d_proj, w_two.T, preferred_element_type=jnp.float32)).astype(jnp.bfloat16)
    d_w_two = jnp.dot(hidden.T, d_proj, preferred_element_type=jnp.float32)
    return token_loss, total_loss, d_hidden, d_embed, d_w_two, d_ln_scale, d_ln_shift
```

```python
import functools
import math

import jax
import jax.numpy as jnp
from jax import lax
from jax.experimental import pallas as pl
from jax.experimental.pallas import tpu as pltpu
from jax.sharding import PartitionSpec as P

LN_EPS = 1e-5
CORES = 2
SIDE = 4
F32 = jnp.float32
BF16 = jnp.bfloat16
MESH = pl.DeviceIdType.MESH
DIRS = (1, -1)


def guarded(cond, fn):
    if isinstance(cond, bool):
        if cond:
            fn()
    else:
        pl.when(cond)(fn)


def both(a, b):
    return a and b if isinstance(a, bool) else a & b


def layer_norm(values, gain, bias):
    mean_val = jnp.mean(values, axis=-1, keepdims=True)
    centered = values - mean_val
    variance = jnp.mean(centered * centered, axis=-1, keepdims=True)
    return centered * lax.rsqrt(variance + LN_EPS) * gain + bias


def dot(a, b, ca, cb):
    return lax.dot_general(a, b, (((ca,), (cb,)), ((), ())), preferred_element_type=F32)


def fused_kernel(nq, info_ref, hid_ref, w2_ref, gain_ref, bias_ref, emb_ref,
                 dx_out, de_out, loss_out, cnt_out,
                 e_all, d_e, zt, dzt, x_new, x_next, x_cur, h_all, w2, d_x, r1, r2, r3, r4,
                 info_all, tgt_v, wgt_v, msk_v, cnt, stat_s, stat_r, m_v, s_v, lse_l, lse_v, tgt_a, tgt_p, loss_v, loss_p,
                 load_sem, ag_s, ag_r, rs_s, rs_r, st_s, st_r, misc_s, misc_r, free_sem):
    nch = 2 * nq
    rows = emb_ref.shape[0]
    vocab = e_all.shape[0]
    dim = e_all.shape[1]
    half = dim // 2
    quart = dim // 4
    chips, blk = SIDE * SIDE, h_all.shape[3]
    rpc = chips * blk
    me = lax.axis_index('tp')
    core = lax.rem(me, CORES)
    chip = lax.div(me, CORES)
    yy = lax.div(chip, SIDE)
    xx = lax.rem(chip, SIDE)

    def wrap(v):
        return lax.rem(v + 2 * SIDE, SIDE)

    def dev(y, x, c):
        return {'tp': (y * SIDE + x) * CORES + c}

    partner = dev(yy, xx, 1 - core)
    peers = [dev(wrap(yy + dy), wrap(xx + dx), core) for dy in range(SIDE) for dx in range(SIDE) if dy or dx]

    def neighbour(axis, d):
        return dev(yy, wrap(xx + d), core) if axis == 0 else dev(wrap(yy + d), xx, core)

    def remote(src, dst, ssem, rsem, target):
        return pltpu.make_async_remote_copy(src_ref=src, dst_ref=dst, send_sem=ssem, recv_sem=rsem,
                                            device_id=target, device_id_type=MESH)

    my_rows = pl.ds(pl.multiple_of(core * rows, 128), rows)
    other_rows = pl.ds(pl.multiple_of((1 - core) * rows, 128), rows)
    load_e = pltpu.make_async_copy(emb_ref, e_all.at[my_rows], load_sem.at[0])
    load_w = pltpu.make_async_copy(w2_ref, w2, load_sem.at[1])
    load_h = [pltpu.make_async_copy(hid_ref.at[pl.ds(q * blk, blk)], h_all.at[q, yy, xx], load_sem.at[2 + q])
              for q in range(nq)]
    for c in load_h:
        c.start()
    load_e.start()
    load_w.start()

    barrier = pltpu.get_barrier_semaphore()
    for t in peers + [partner]:
        pl.semaphore_signal(barrier, inc=1, device_id=t, device_id_type=MESH)
    pl.semaphore_wait(barrier, len(peers) + 1)

    def line(h, q, pos1, pos2, cols):
        px, py = (pos1, pos2) if h == 0 else (pos2, pos1)
        py = slice(None) if py is None else py
        px = slice(None) if px is None else px
        return h_all.at[q, py, px, :, cols]

    def coords(h):
        return (xx, yy) if h == 0 else (yy, xx)

    def sub(h, d):
        return pl.ds(h * half + (0 if d == 1 else quart), quart)

    def cols_of(h):
        return pl.ds(h * half, half)

    def ag_copy(step, h, q, d):
        a, b = coords(h)
        axis = h if step < 2 else 1 - h
        if step == 0:
            r = line(h, q, a, b, cols_of(h))
        elif step == 1:
            r = line(h, q, wrap(a - d), b, sub(h, d))
        elif step == 2:
            r = line(h, q, None, b, cols_of(h))
        else:
            r = line(h, q, None, wrap(b - d), sub(h, d))
        return remote(r, r, ag_s.at[q, step, h, 0 if d == 1 else 1], ag_r.at[q, step, h, 0 if d == 1 else 1],
                      neighbour(axis, d))

    def ag_start(step, q):
        for h in range(2):
            for d in DIRS:
                ag_copy(step, h, q, d).start()

    def ag_wait_recv(step, q):
        for h in range(2):
            for d in DIRS:
                a, b = coords(h)
                if step == 0:
                    r = line(h, q, wrap(a - d), b, cols_of(h))
                elif step == 1:
                    r = line(h, q, wrap(a - 2 * d), b, sub(h, d))
                elif step == 2:
                    r = line(h, q, None, wrap(b - d), cols_of(h))
                else:
                    r = line(h, q, None, wrap(b - 2 * d), sub(h, d))
                k = 0 if d == 1 else 1
                remote(r, r, ag_s.at[q, step, h, k], ag_r.at[q, step, h, k], partner).wait_recv()

    def ag_tick(k):
        for step in (3, 2, 1, 0):
            q = k - step

            def go(step=step, q=q):
                if step > 0:
                    ag_wait_recv(step - 1, q)
                ag_start(step, q)
            guarded(both(q >= 0, q < nq), go)

    def ag_finish(q):
        ag_wait_recv(3, q)
        for step in range(4):
            for h in range(2):
                for d in DIRS:
                    ag_copy(step, h, q, d).wait_send()

    for c in load_h:
        c.wait()
    ag_tick(0)

    info_copies = [remote(info_ref, info_all.at[chip], misc_s.at[0], misc_r.at[0], t) for t in peers]
    for c in info_copies:
        c.start()
    info_all[chip] = info_ref[...]
    load_e.wait()
    send_e = remote(e_all.at[my_rows], e_all.at[my_rows], misc_s.at[1], misc_r.at[1], partner)
    send_e.start()
    ag_tick(1)
    zt[...] = jnp.zeros(zt.shape, F32)
    d_e[...] = jnp.zeros(d_e.shape, F32)
    ag_tick(2)
    every_info = info_all.at[pl.ds(0, chips - 1)]
    remote(every_info, every_info, misc_s.at[0], misc_r.at[0], partner).wait_recv()
    remote(every_info, every_info, misc_s.at[0], misc_r.at[0], partner).wait_send()
    total = jnp.zeros((8, rpc), F32)
    for q in range(nq):
        got = jnp.concatenate([info_all[o][:, q * blk:(q + 1) * blk] for o in range(chips)], axis=1)
        total = total + got
        for hd in range(2):
            c = (1 - hd) * nq + q
            tgt_v[c] = got[hd:hd + 1].astype(jnp.int32) - chip * vocab
            msk_v[c] = got[2 + hd:3 + hd]
    cnt[0] = jnp.broadcast_to(jnp.sum(total, axis=1, keepdims=True), cnt.shape[1:])
    send_c = remote(cnt.at[0], cnt.at[1], misc_s.at[2], misc_r.at[2], partner)
    send_c.start()
    ag_tick(3)
    send_c.wait()
    counts = cnt[0] + cnt[1]
    for hd in range(2):
        for q in range(nq):
            c = (1 - hd) * nq + q
            wgt_v[c] = msk_v[c] / counts[2 + hd:3 + hd, 0:1]
    load_w.wait()

    def part(slot, h, pos1, pos2, cols):
        px, py = (pos1, pos2) if h == 0 else (pos2, pos1)
        py = slice(None) if py is None else py
        px = slice(None) if px is None else px
        return d_x.at[slot, py, px, :, cols]

    def rs_copy(step, slot, h, d):
        a, b = coords(h)
        k = 0 if d == 1 else 1
        if step == 0:
            src, dst = part(slot, h, wrap(a + 2), None, sub(h, d)), r1.at[slot, h, k]
        elif step == 1:
            src, dst = part(slot, h, wrap(a + d), None, cols_of(h)), r2.at[slot, h, k]
        elif step == 2:
            src, dst = part(slot, h, a, wrap(b + 2), sub(h, d)), r3.at[slot, h, k]
        else:
            src, dst = part(slot, h, a, wrap(b + d), cols_of(h)), r4.at[slot, h, k]
        return remote(src, dst, rs_s.at[slot, step, h, k], rs_r.at[slot, step, h, k],
                      neighbour(h if step < 2 else 1 - h, d))

    def rs_step(step, h, c):
        slot = c % 3 if isinstance(c, int) else lax.rem(c + 3, 3)
        a, b = coords(h)

        def go():
            if step > 0:
                for d in DIRS:
                    rs_copy(step - 1, slot, h, d).wait_recv()
            if step == 1:
                for k, d in enumerate(DIRS):
                    r = part(slot, h, wrap(a + d), None, sub(h, d))
                    r[...] = r[...] + r1[slot, h, k]
            elif step == 2:
                r = part(slot, h, a, None, cols_of(h))
                r[...] = r[...] + r2[slot, h, 0] + r2[slot, h, 1]
            elif step == 3:
                for k, d in enumerate(DIRS):
                    r = part(slot, h, a, wrap(b + d), sub(h, d))
                    r[...] = r[...] + r3[slot, h, k]
            elif step == 4:
                r = part(slot, h, a, b, cols_of(h))
                dx_out[c, :, h * half:(h + 1) * half] = r[...] + r4[slot, h, 0] + r4[slot, h, 1]
            if step < 4:
                for d in DIRS:
                    rs_copy(step, slot, h, d).start()
            else:
                for s in range(4):
                    for d in DIRS:
                        rs_copy(s, slot, h, d).wait_send()
        guarded(both(c >= 0, c < nch), go)

    def stat_copies(par):
        return [remote(stat_s.at[par], stat_r.at[par, chip], st_s.at[par], st_r.at[par], t) for t in peers]

    def stat_send(e):
        par = e % 2 if isinstance(e, int) else lax.rem(e, 2)

        @pl.when(e >= 2)
        def _():
            drain = stat_r.at[par, pl.ds(0, chips - 1)]
            remote(drain, drain, st_s.at[par], st_r.at[par], partner).wait_send()
        stat_s[par, 0:1, :] = lse_l[...]
        stat_s[par, 1:2, :] = tgt_p[...]
        stat_r[par, chip] = stat_s[par]
        for c in stat_copies(par):
            c.start()

    def stat_wait(e):
        par = e % 2 if isinstance(e, int) else lax.rem(e, 2)
        drain = stat_r.at[par, pl.ds(0, chips - 1)]
        remote(drain, drain, st_s.at[par], st_r.at[par], partner).wait_recv()
        got = stat_r[par]
        lse = got[:, 0, :]
        top = jnp.max(lse, axis=0, keepdims=True)
        new_lse = top + jnp.log(jnp.sum(jnp.exp(lse - top), axis=0, keepdims=True))

        def put():
            loss_v[e - 1] = (lse_v[...] - jnp.sum(got[:, 1, :], axis=0, keepdims=True)) * msk_v[e - 1]
        guarded(e >= 1, put)
        lse_v[...] = new_lse

    tile = 256

    def project(q):
        h = h_all[q].reshape(rpc, dim)
        for n0 in range(0, dim, half):
            x_new[:, n0:n0 + half] = dot(h, w2[:, n0:n0 + half], 1, 0).astype(BF16)

    def norm_rows(two, q, lo, hi):
        step, per = 64, blk * SIDE
        hd = 1 if two else 0
        for r in range(lo, hi, step):
            if two:
                val = x_new[r:r + step, :]
            else:
                val = h_all[q, r // per, (r % per) // blk:(r % per + step) // blk].reshape(step, dim)
            val = layer_norm(val.astype(F32), gain_ref[hd:hd + 1, :], bias_ref[hd:hd + 1, :])
            x_new[r:r + step, :] = val.astype(BF16)

    def logits_tile(v0, top):
        z = dot(e_all[v0:v0 + tile, :], x_next[...], 1, 1)
        zt[v0:v0 + tile, :] = z
        return jnp.maximum(top, jnp.max(z.reshape(tile // 8, 8, rpc), axis=0))

    def grad_tile(v0, lse, tgt, wgt, acc):
        z = zt[v0:v0 + tile, :]
        ids = lax.broadcasted_iota(jnp.int32, (tile, rpc), 0)
        hit = ids == tgt - v0
        acc = acc + jnp.sum(jnp.where(hit, z, 0.0).reshape(tile // 8, 8, rpc), axis=0)
        prob = jnp.exp(z - lse)
        dzt[v0:v0 + tile, :] = (jnp.where(hit, prob - 1.0, prob) * wgt).astype(BF16)
        return acc

    n_tiles = vocab // tile
    mid = n_tiles // 2 + 1

    def phase_one(i, lo, hi, with_logits):
        c = jnp.maximum(i, 0)
        lse, tgt, wgt = lse_v[...], tgt_v[c], wgt_v[c]
        top = m_v[...] if lo else jnp.full((8, rpc), -jnp.inf, F32)
        acc = tgt_a[...] if lo else jnp.zeros((8, rpc), F32)
        for j in range(lo, hi):
            acc = grad_tile(j * tile, lse, tgt, wgt, acc)
            if with_logits:
                top = logits_tile(j * tile, top)
        if with_logits:
            m_v[...] = top
        tgt_a[...] = acc
        if hi == n_tiles:
            tgt_p[...] = jnp.sum(acc, axis=0, keepdims=True)

    def dx_half(slot, h):
        val = dot(dzt[...], e_all[:, h * half:(h + 1) * half], 0, 0)
        d_x[slot, :, :, :, h * half:(h + 1) * half] = val.reshape(SIDE, SIDE, blk, half)

    def exp_pass():
        top = jnp.max(m_v[...], axis=0, keepdims=True)
        acc = jnp.zeros((8, rpc), F32)
        for j in range(n_tiles):
            prob = jnp.exp(zt[j * tile:(j + 1) * tile, :] - top)
            acc = acc + jnp.sum(prob.reshape(tile // 8, 8, rpc), axis=0)
        lse_l[...] = top + jnp.log(jnp.sum(acc, axis=0, keepdims=True))

    de_tile = rows // 4

    def phase_three(i, second, with_grad, two, q):
        base = (core if second else 1 - core) * rows
        lo = rpc // 2 if second else 0
        if two:
            if not second:
                project(q)
            else:
                norm_rows(True, q, 0, rpc)
        else:
            norm_rows(False, q, lo, lo + rpc // 2)
        if with_grad:
            for j in range(4):
                r = pl.ds(pl.multiple_of(base + j * de_tile, 32), de_tile)
                d_e[r, :] = d_e[r, :] + dot(dzt[r, :], x_cur[...], 1, 0)

    def three(i, second):
        q = lax.rem(i + 2, nq)
        pl.when(i < 0)(lambda: phase_three(i, second, False, True, q))
        pl.when((i >= 0) & (i < nq - 2))(lambda: phase_three(i, second, True, True, q))
        pl.when(i >= nq - 2)(lambda: phase_three(i, second, True, False, q))

    def give(h):
        lanes = slice(h * half, (h + 1) * half)
        return remote(d_e.at[other_rows, lanes], zt.at[pl.ds(h * rows, rows)], misc_s.at[3 + h], misc_r.at[3 + h], partner)

    m_v[...] = jnp.zeros(m_v.shape, F32)
    lse_v[...] = jnp.zeros(lse_v.shape, F32)
    lse_l[...] = jnp.zeros(lse_l.shape, F32)
    remote(e_all.at[other_rows], e_all.at[other_rows], misc_s.at[1], misc_r.at[1], partner).wait()

    def chunk(i, carry):
        slot = lax.rem(i + 3, 3)
        last = i == nch - 1
        pl.when(i >= 0)(lambda: stat_wait(i))
        pl.when((i >= -1) & (i < nch - 1))(lambda: phase_one(i, 0, mid, True))
        pl.when(last)(lambda: phase_one(i, 0, mid, False))
        rs_step(1, 1, i - 1)
        rs_step(3, 1, i - 2)
        pl.when((i >= -1) & (i < nch - 1))(lambda: phase_one(i, mid, n_tiles, True))
        pl.when(last)(lambda: phase_one(i, mid, n_tiles, False))
        pl.when(last)(lambda: pl.semaphore_signal(free_sem, inc=1, device_id=partner, device_id_type=MESH))
        rs_step(4, 0, i - 2)
        pl.when(i >= -1)(lambda: ag_tick(2 * i + 7))

        @pl.when(i == -1)
        def _():
            exp_pass()

        @pl.when((i >= 0) & (i < nch - 1))
        def _():
            dx_half(slot, 0)
            exp_pass()

        @pl.when(last)
        def _():
            dx_half(slot, 0)
        pl.when(i >= -1)(lambda: stat_send(i + 1))
        rs_step(0, 0, i)
        rs_step(4, 1, i - 2)
        pl.when(i >= 0)(lambda: dx_half(slot, 1))
        rs_step(0, 1, i)
        rs_step(2, 0, i - 1)
        pl.when(i < nq - 2)(lambda: ag_finish(i + 2))
        three(i, False)

        @pl.when(last)
        def _():
            pl.semaphore_wait(free_sem, 1)
            for h in range(2):
                give(h).start()
        rs_step(2, 1, i - 1)
        three(i, True)
        rs_step(1, 0, i)
        rs_step(3, 0, i - 1)
        ag_tick(2 * i + 8)
        x_cur[...] = x_next[...]
        x_next[...] = x_new[...]
        return carry

    lax.fori_loop(-2, nch, chunk, 0)

    c = nch - 1
    rs_step(1, 1, c)
    rs_step(3, 1, c - 1)
    rs_step(4, 0, c - 1)
    rs_step(4, 1, c - 1)
    stat_wait(nch)
    send_l = remote(loss_v, loss_p, misc_s.at[5], misc_r.at[5], partner)
    send_l.start()
    rs_step(2, 0, c)
    rs_step(2, 1, c)
    for h in range(2):
        give(h).wait()
    outs = []
    out_tile = rows // 8
    for j in range(8):
        r = pl.ds(pl.multiple_of(core * rows + j * out_tile, 8), out_tile)
        for h in range(2):
            lanes = slice(h * half, (h + 1) * half)
            d_e[r, lanes] = d_e[r, lanes] + zt[h * rows + j * out_tile:h * rows + (j + 1) * out_tile, :]
        outs.append(pltpu.make_async_copy(d_e.at[r], de_out.at[pl.ds(j * out_tile, out_tile)], load_sem.at[j]))
        outs[-1].start()
    rs_step(3, 0, c)
    rs_step(3, 1, c)
    send_l.wait()
    loss_out[core] = loss_v[...]
    loss_out[1 - core] = loss_p[...]
    cnt_out[...] = counts
    for par in range(2):
        drain = stat_r.at[par, pl.ds(0, chips - 1)]
        remote(drain, drain, st_s.at[par], st_r.at[par], partner).wait_send()
    rs_step(4, 0, c)
    rs_step(4, 1, c)
    for o in outs:
        o.wait()


def solution(mesh):
    tok_spec = P(('dp', 'tp'), None)
    row_spec = P(None, ('dp', 'tp'))
    chips = mesh.shape['tp'] // CORES
    assert math.isqrt(chips) == SIDE

    def run_kernel(info, hidden, w_two, gain, bias, embed):
        tok, dim = hidden.shape
        rows = embed.shape[0]
        blk = 32
        nq = tok // blk
        nch, rpc, half, quart = 2 * nq, chips * blk, dim // 2, dim // 4
        vocab = CORES * rows
        vmem = pl.BlockSpec(memory_space=pltpu.VMEM)
        hbm = pl.BlockSpec(memory_space=pltpu.MemorySpace.HBM)
        dma = pltpu.SemaphoreType.DMA
        return pl.pallas_call(
            functools.partial(fused_kernel, nq),
            out_shape=(jax.ShapeDtypeStruct((nch, blk, dim), F32), jax.ShapeDtypeStruct((rows, dim), F32),
                       jax.ShapeDtypeStruct((CORES, nch, 1, rpc), F32), jax.ShapeDtypeStruct((8, 128), F32)),
            in_specs=[vmem, hbm, hbm, vmem, vmem, hbm],
            out_specs=[vmem, hbm, vmem, vmem],
            scratch_shapes=[
                pltpu.VMEM((vocab, dim), BF16), pltpu.VMEM((vocab, dim), F32),
                pltpu.VMEM((vocab, rpc), F32), pltpu.VMEM((vocab, rpc), BF16),
                pltpu.VMEM((rpc, dim), BF16), pltpu.VMEM((rpc, dim), BF16), pltpu.VMEM((rpc, dim), BF16),
                pltpu.VMEM((nq, SIDE, SIDE, blk, dim), BF16), pltpu.VMEM((dim, dim), BF16),
                pltpu.VMEM((3, SIDE, SIDE, blk, dim), F32),
                pltpu.VMEM((3, 2, 2, SIDE, blk, quart), F32), pltpu.VMEM((3, 2, 2, SIDE, blk, half), F32),
                pltpu.VMEM((3, 2, 2, blk, quart), F32), pltpu.VMEM((3, 2, 2, blk, half), F32),
                pltpu.VMEM((chips, 8, tok), F32), pltpu.VMEM((nch, 1, rpc), jnp.int32),
                pltpu.VMEM((nch, 1, rpc), F32), pltpu.VMEM((nch, 1, rpc), F32), pltpu.VMEM((2, 8, 128), F32),
                pltpu.VMEM((2, 2, rpc), F32), pltpu.VMEM((2, chips, 2, rpc), F32),
                pltpu.VMEM((8, rpc), F32), pltpu.VMEM((8, rpc), F32), pltpu.VMEM((1, rpc), F32),
                pltpu.VMEM((1, rpc), F32), pltpu.VMEM((8, rpc), F32), pltpu.VMEM((1, rpc), F32),
                pltpu.VMEM((nch, 1, rpc), F32), pltpu.VMEM((nch, 1, rpc), F32),
                dma((2 + nq,)), dma((nq, 4, 2, 2)), dma((nq, 4, 2, 2)), dma((3, 4, 2, 2)), dma((3, 4, 2, 2)),
                dma((2,)), dma((2,)), dma((6,)), dma((6,)), pltpu.SemaphoreType.REGULAR,
            ],
            compiler_params=pltpu.CompilerParams(collective_id=0, has_side_effects=True,
                                                 vmem_limit_bytes=63 * 1024 * 1024),
            name='fused_heads',
        )(info, hidden, w_two, gain, bias, embed)

    def device_step(hidden, w_two, ln_scale, ln_shift, embed, targets, loss_mask):
        tok, dim = hidden.shape
        me = lax.axis_index('tp')
        info = jnp.concatenate([targets, loss_mask, jnp.zeros((4, tok), jnp.int32)]).astype(F32)
        dx, d_embed, losses, counts = run_kernel(info, hidden, w_two, ln_scale, ln_shift, embed)
        dx_loc = dx.reshape(2, tok, dim)[::-1]
        losses = losses.reshape(CORES, 2, tok // 32, chips, 32)[:, ::-1]
        mine = lax.dynamic_index_in_dim(losses, me % CORES, 0, keepdims=False)
        token_loss = lax.dynamic_index_in_dim(mine, me // CORES, 2, keepdims=False).reshape(2, tok)
        total_loss = jnp.sum(jnp.sum(losses, axis=(0, 2, 3, 4)) / counts[2:4, 0]).reshape(1)
        proj_out = jnp.dot(hidden, w_two, preferred_element_type=F32).astype(BF16)
        norm_input = jnp.stack([hidden.astype(F32), proj_out.astype(F32)])
        _, ln_back = jax.vjp(jax.vmap(layer_norm), norm_input, ln_scale, ln_shift)
        d_norm_in, d_scale_part, d_shift_part = ln_back(dx_loc)
        d_proj = d_norm_in[1].astype(BF16)
        d_hidden = (d_norm_in[0] + jnp.einsum('td,ed->te', d_proj, w_two, preferred_element_type=F32)).astype(BF16)
        d_w_part = jnp.einsum('te,td->ed', hidden, d_proj, preferred_element_type=F32)
        d_w_two, d_scale, d_shift = lax.psum((d_w_part, d_scale_part, d_shift_part), 'tp')
        return token_loss, total_loss, d_hidden, d_embed, d_w_two, d_scale, d_shift

    return jax.shard_map(device_step, mesh=mesh,
                         in_specs=(tok_spec, P(), P(), P(), P('tp', None), row_spec, row_spec),
                         out_specs=(row_spec, P('dp'), tok_spec, tok_spec, P('dp', None), P('dp', None), P('dp', None)),
                         check_vma=False)
```

```python
import functools
import math

import jax
import jax.numpy as jnp
from jax import lax
from jax.experimental import pallas as pl
from jax.experimental.pallas import tpu as pltpu
from jax.sharding import PartitionSpec as P

LN_EPS = 1e-5
BIG = 1e30
CORES = 2
SIDE = 4
BLOCK = 32
VMEM_BYTES = 67043328
F32 = jnp.float32
BF16 = jnp.bfloat16
MESH = pl.DeviceIdType.MESH
DIRS = (1, -1)


def guarded(cond, fn):
    if isinstance(cond, bool):
        if cond:
            fn()
    else:
        pl.when(cond)(fn)


def both(a, b):
    return a and b if isinstance(a, bool) else a & b


def layer_norm(values, gain, bias):
    mean_val = jnp.mean(values, axis=-1, keepdims=True)
    centered = values - mean_val
    variance = jnp.mean(centered * centered, axis=-1, keepdims=True)
    return centered * lax.rsqrt(variance + LN_EPS) * gain + bias


def dot(a, b, ca, cb):
    return lax.dot_general(a, b, (((ca,), (cb,)), ((), ())), preferred_element_type=F32)


def fused_kernel(nq, info_ref, hid_ref, w2_ref, gain_ref, bias_ref, emb_ref,
                 dh_out, de_out, dw_out, hop, ln_out, loss_out, cnt_out,
                 e_all, d_e, zt, dzt, x_new, x_next, x_cur, h_all, w2, d_x, r1, r2, r3, r4,
                 info_all, tgt_v, wgt_v, msk_v, cnt, stat_s, stat_r, m_v, lse_l, lse_v, tgt_l, loss_v, loss_p,
                 dx_own, dw_part, dw_own, ln_s, ln_r, ln_p,
                 load_sem, ag_s, ag_r, rs_s, rs_r, st_s, st_r, misc_s, misc_r, lx_s, lx_r, wg_s, wg_r, free_sem):
    nch = 2 * nq
    rows = emb_ref.shape[0]
    vocab = e_all.shape[0]
    dim = e_all.shape[1]
    half = dim // 2
    quart = dim // 4
    chips, blk = SIDE * SIDE, h_all.shape[3]
    tok = nq * blk
    extra = nq + 2
    rpc = chips * blk
    me = lax.axis_index('tp')
    core = lax.rem(me, CORES)
    chip = lax.div(me, CORES)
    yy = lax.div(chip, SIDE)
    xx = lax.rem(chip, SIDE)

    def wrap(v):
        return lax.rem(v + 2 * SIDE, SIDE)

    def dev(y, x, c):
        return {'tp': (y * SIDE + x) * CORES + c}

    partner = dev(yy, xx, 1 - core)
    peers = [dev(wrap(yy + dy), wrap(xx + dx), core) for dy in range(SIDE) for dx in range(SIDE) if dy or dx]

    def neighbour(axis, d):
        return dev(yy, wrap(xx + d), core) if axis == 0 else dev(wrap(yy + d), xx, core)

    def remote(src, dst, ssem, rsem, target):
        return pltpu.make_async_remote_copy(src_ref=src, dst_ref=dst, send_sem=ssem, recv_sem=rsem,
                                            device_id=target, device_id_type=MESH)

    my_rows = pl.ds(pl.multiple_of(core * rows, 128), rows)
    other_rows = pl.ds(pl.multiple_of((1 - core) * rows, 128), rows)
    load_e = pltpu.make_async_copy(emb_ref, e_all.at[my_rows], load_sem.at[0])
    load_w = pltpu.make_async_copy(w2_ref, w2, load_sem.at[1])
    load_h = [pltpu.make_async_copy(hid_ref.at[pl.ds(q * blk, blk)], h_all.at[q, yy, xx], load_sem.at[2 + q])
              for q in range(nq)]
    for c in load_h:
        c.start()
    load_e.start()
    load_w.start()

    barrier = pltpu.get_barrier_semaphore()
    for t in peers + [partner]:
        pl.semaphore_signal(barrier, inc=1, device_id=t, device_id_type=MESH)
    pl.semaphore_wait(barrier, len(peers) + 1)

    def coords(h):
        return (xx, yy) if h == 0 else (yy, xx)

    def sub(h, d):
        return pl.ds(h * half + (0 if d == 1 else quart), quart)

    def cols_of(h):
        return pl.ds(h * half, half)

    def gathered(buf, step, h, d, back):
        a, b = coords(h)
        if step == 0:
            pos, cols = (wrap(a - back * d), b), cols_of(h)
        elif step == 1:
            pos, cols = (wrap(a - (1 + back) * d), b), sub(h, d)
        elif step == 2:
            pos, cols = (None, wrap(b - back * d)), cols_of(h)
        else:
            pos, cols = (None, wrap(b - (1 + back) * d)), sub(h, d)
        px, py = pos if h == 0 else pos[::-1]
        py = slice(None) if py is None else py
        px = slice(None) if px is None else px
        return buf.at[py, px, :, cols]

    def ag_copy(step, h, q, d, back=0):
        k = 0 if d == 1 else 1
        r = gathered(h_all.at[q], step, h, d, back)
        return remote(r, r, ag_s.at[q, step, h, k], ag_r.at[q, step, h, k],
                      neighbour(h if step < 2 else 1 - h, d))

    def ag_start(step, q):
        for h in range(2):
            for d in DIRS:
                ag_copy(step, h, q, d).start()

    def ag_wait_recv(step, q):
        for h in range(2):
            for d in DIRS:
                ag_copy(step, h, q, d, 1).wait_recv()

    def ag_tick(k):
        for step in (3, 2, 1, 0):
            q = k - step

            def go(step=step, q=q):
                if step > 0:
                    ag_wait_recv(step - 1, q)
                ag_start(step, q)
            guarded(both(q >= 0, q < nq), go)

    def ag_finish(q):
        ag_wait_recv(3, q)
        for step in range(4):
            for h in range(2):
                for d in DIRS:
                    ag_copy(step, h, q, d).wait_send()

    for c in load_h:
        c.wait()
    ag_tick(0)

    info_copies = [remote(info_ref, info_all.at[chip], misc_s.at[0], misc_r.at[0], t) for t in peers]
    for c in info_copies:
        c.start()
    info_all[chip] = info_ref[...]
    load_e.wait()
    send_e = remote(e_all.at[my_rows], e_all.at[my_rows], misc_s.at[1], misc_r.at[1], partner)
    send_e.start()
    ag_tick(1)
    ag_tick(2)
    every_info = info_all.at[pl.ds(0, chips - 1)]
    remote(every_info, every_info, misc_s.at[0], misc_r.at[0], partner).wait_recv()
    remote(every_info, every_info, misc_s.at[0], misc_r.at[0], partner).wait_send()
    total = jnp.zeros((8, rpc), F32)
    for q in range(nq):
        got = jnp.concatenate([info_all[o][:, q * blk:(q + 1) * blk] for o in range(chips)], axis=1)
        total = total + got
        for hd in range(2):
            c = (1 - hd) * nq + q
            tgt_v[c] = got[hd:hd + 1].astype(jnp.int32) - chip * vocab
            msk_v[c] = got[2 + hd:3 + hd]
    cnt[0] = jnp.broadcast_to(jnp.sum(total, axis=1, keepdims=True), cnt.shape[1:])
    send_c = remote(cnt.at[0], cnt.at[1], misc_s.at[2], misc_r.at[2], partner)
    send_c.start()
    ag_tick(3)
    send_c.wait()
    counts = cnt[0] + cnt[1]
    for hd in range(2):
        for q in range(nq):
            c = (1 - hd) * nq + q
            wgt_v[c] = msk_v[c] / counts[2 + hd:3 + hd, 0:1]
    load_w.wait()

    def part(slot, h, pos1, pos2, cols):
        px, py = (pos1, pos2) if h == 0 else (pos2, pos1)
        py = slice(None) if py is None else py
        px = slice(None) if px is None else px
        return d_x.at[slot, py, px, :, cols]

    def rs_copy(step, slot, h, d):
        a, b = coords(h)
        k = 0 if d == 1 else 1
        if step == 0:
            src, dst = part(slot, h, wrap(a + 2), None, sub(h, d)), r1.at[slot, h, k]
        elif step == 1:
            src, dst = part(slot, h, wrap(a + d), None, cols_of(h)), r2.at[slot, h, k]
        elif step == 2:
            src, dst = part(slot, h, a, wrap(b + 2), sub(h, d)), r3.at[slot, h, k]
        else:
            src, dst = part(slot, h, a, wrap(b + d), cols_of(h)), r4.at[slot, h, k]
        return remote(src, dst, rs_s.at[slot, step, h, k], rs_r.at[slot, step, h, k],
                      neighbour(h if step < 2 else 1 - h, d))

    def rs_step(step, h, c):
        slot = c % 3 if isinstance(c, int) else lax.rem(c + 3, 3)
        a, b = coords(h)

        def go():
            if step > 0:
                for d in DIRS:
                    rs_copy(step - 1, slot, h, d).wait_recv()
            if step == 1:
                for k, d in enumerate(DIRS):
                    r = part(slot, h, wrap(a + d), None, sub(h, d))
                    r[...] = r[...] + r1[slot, h, k]
            elif step == 2:
                r = part(slot, h, a, None, cols_of(h))
                r[...] = r[...] + r2[slot, h, 0] + r2[slot, h, 1]
            elif step == 3:
                for k, d in enumerate(DIRS):
                    r = part(slot, h, a, wrap(b + d), sub(h, d))
                    r[...] = r[...] + r3[slot, h, k]
            elif step == 4:
                r = part(slot, h, a, b, cols_of(h))
                val = r[...] + r4[slot, h, 0] + r4[slot, h, 1]

                def keep_dx():
                    at = c - 1 if isinstance(c, int) else jnp.where(c < extra, c, c - 1)
                    dx_own[at, :, h * half:(h + 1) * half] = val

                def keep_dw():
                    dw_own[:, h * half:(h + 1) * half] = val
                guarded(c != extra, keep_dx)
                guarded(c == extra, keep_dw)
            if step < 4:
                for d in DIRS:
                    rs_copy(step, slot, h, d).start()
            else:
                for s in range(4):
                    for d in DIRS:
                        rs_copy(s, slot, h, d).wait_send()
        guarded(both(c >= 0, c <= nch), go)

    def stat_drain(par):
        drain = stat_r.at[par, pl.ds(0, chips - 1)]
        return remote(drain, drain, st_s.at[par], st_r.at[par], partner)

    def stat_send(e):
        par = lax.rem(e, 2)
        pl.when(e >= 2)(lambda: stat_drain(par).wait_send())
        stat_s[par, 0:1, :] = lse_l[...]
        stat_s[par, 1:2, :] = tgt_l[...]
        stat_r[par, chip] = stat_s[par]
        for t in peers:
            remote(stat_s.at[par], stat_r.at[par, chip], st_s.at[par], st_r.at[par], t).start()

    def stat_wait(e):
        par = lax.rem(e, 2)
        stat_drain(par).wait_recv()
        got = stat_r[par]
        lse = got[:, 0, :]
        top = jnp.max(lse, axis=0, keepdims=True)
        lse = top + jnp.log(jnp.sum(jnp.exp(lse - top), axis=0, keepdims=True))
        loss_v[e] = (lse - jnp.sum(got[:, 1, :], axis=0, keepdims=True)) * msk_v[e]
        wgt = wgt_v[e]
        live = wgt > 0.0
        lse_v[...] = jnp.where(live, lse - jnp.log(jnp.where(live, wgt, 1.0)), BIG)

    tile = 256

    def project(q):
        h = h_all[q].reshape(rpc, dim)
        for n0 in range(0, dim, half):
            x_new[:, n0:n0 + half] = dot(h, w2[:, n0:n0 + half], 1, 0).astype(BF16)

    def norm_rows(two, q, lo, hi):
        step, per = 64, blk * SIDE
        hd = 1 if two else 0
        for r in range(lo, hi, step):
            if two:
                val = x_new[r:r + step, :]
            else:
                val = h_all[q, r // per, (r % per) // blk:(r % per + step) // blk].reshape(step, dim)
            val = layer_norm(val.astype(F32), gain_ref[hd:hd + 1, :], bias_ref[hd:hd + 1, :])
            x_new[r:r + step, :] = val.astype(BF16)

    def logits_tile(v0, top):
        z = dot(e_all[v0:v0 + tile, :], x_next[...], 1, 1)
        zt[v0:v0 + tile, :] = z
        return jnp.maximum(top, jnp.max(z.reshape(tile // 8, 8, rpc), axis=0))

    def grad_tile(v0, shift, tgt, wgt):
        prob = jnp.exp(zt[v0:v0 + tile, :] - shift)
        hit = lax.broadcasted_iota(jnp.int32, (tile, rpc), 0) == tgt - v0
        dzt[v0:v0 + tile, :] = jnp.where(hit, prob - wgt, prob).astype(BF16)

    n_tiles = vocab // tile
    mid = n_tiles // 2 + 1

    def phase_one(c, lo, hi, with_logits):
        at = jnp.maximum(c, 0)
        shift, tgt, wgt = lse_v[...], tgt_v[at], wgt_v[at]
        top = m_v[...] if lo else jnp.full((8, rpc), -jnp.inf, F32)
        for j in range(lo, hi):
            grad_tile(j * tile, shift, tgt, wgt)
            if with_logits:
                top = logits_tile(j * tile, top)
        if with_logits:
            m_v[...] = top

    def dx_half(slot, h):
        val = dot(dzt[...], e_all[:, h * half:(h + 1) * half], 0, 0)
        d_x[slot, :, :, :, h * half:(h + 1) * half] = val.reshape(SIDE, SIDE, blk, half)

    def exp_pass(c, slot, with_dx):
        top = jnp.max(m_v[...], axis=0, keepdims=True)
        tgt = tgt_v[c + 1]
        acc = jnp.zeros((8, rpc), F32)
        found = jnp.zeros((8, rpc), F32)
        for j in range(n_tiles):
            if with_dx and j == 9:
                dx_half(slot, 0)
            z = zt[j * tile:(j + 1) * tile, :]
            hit = lax.broadcasted_iota(jnp.int32, (tile, rpc), 0) == tgt - j * tile
            acc = acc + jnp.sum(jnp.exp(z - top).reshape(tile // 8, 8, rpc), axis=0)
            for k in range(0, tile, 8):
                found = jnp.where(hit[k:k + 8], z[k:k + 8], found)
        lse_l[...] = top + jnp.log(jnp.sum(acc, axis=0, keepdims=True))
        tgt_l[...] = jnp.sum(found, axis=0, keepdims=True)

    de_tile = rows // 4

    def phase_three(second, with_grad, two, q):
        base = (core if second else 1 - core) * rows
        lo = rpc // 2 if second else 0
        if not with_grad:
            if not second:
                project(q)
            norm_rows(two, q, lo, lo + rpc // 2)
            return
        for j in range(4):
            norm_rows(two, q, lo + j * rpc // 8, lo + (j + 1) * rpc // 8)
            r = pl.ds(pl.multiple_of(base + j * de_tile, 32), de_tile)
            d_e[r, :] = d_e[r, :] + dot(dzt[r, :], x_cur[...], 1, 0)

    def three(c, second):
        q = lax.rem(c + 2, nq)
        pl.when((c >= -2) & (c < 0))(lambda: phase_three(second, False, True, q))
        if second:
            @pl.when(c == -1)
            def _():
                d_e[...] = jnp.zeros(d_e.shape, F32)
        pl.when((c >= 0) & (c < nq - 2))(lambda: phase_three(second, True, True, q))
        pl.when(c >= nq - 2)(lambda: phase_three(second, True, False, q))

    def own_hidden(j, n, lanes=slice(None)):
        return h_all[j:j + n, yy, xx, :, lanes].reshape(n * blk, -1)

    def norm_back(hd):
        step = 2 * blk
        d_gain = jnp.zeros((8, dim), F32)
        d_bias = jnp.zeros((8, dim), F32)
        if hd == 1:
            for n0 in range(0, dim, half):
                x_new[0:tok, n0:n0 + half] = dot(own_hidden(0, nq), w2[:, n0:n0 + half], 1, 0).astype(BF16)
        for j in range(nq // 2):
            r = j * step
            val = (x_new[r:r + step, :] if hd == 1 else own_hidden(2 * j, 2)).astype(F32)
            cen = val - jnp.mean(val, axis=-1, keepdims=True)
            rstd = lax.rsqrt(jnp.mean(cen * cen, axis=-1, keepdims=True) + LN_EPS)
            hat = cen * rstd
            at = (1 - hd) * nq + 2 * j
            d_y = dx_own[at:at + 2].reshape(step, dim)
            d_gain = d_gain + jnp.sum((d_y * hat).reshape(step // 8, 8, dim), axis=0)
            d_bias = d_bias + jnp.sum(d_y.reshape(step // 8, 8, dim), axis=0)
            g = d_y * gain_ref[hd:hd + 1, :]
            d_in = rstd * (g - jnp.mean(g, axis=-1, keepdims=True) - hat * jnp.mean(g * hat, axis=-1, keepdims=True))
            if hd == 1:
                x_new[tok + r:tok + r + step, :] = d_in.astype(BF16)
            else:
                x_new[r:r + step, :] = (d_in + dx_own[2 * j:2 * j + 2].reshape(step, dim)).astype(BF16)
        ln_s[hd, 0:1, :] = jnp.sum(d_gain, axis=0, keepdims=True)
        ln_s[hd, 1:2, :] = jnp.sum(d_bias, axis=0, keepdims=True)
        ln_r[hd, chip] = ln_s[hd]
        for t in peers:
            remote(ln_s.at[hd], ln_r.at[hd, chip], lx_s.at[hd], lx_r.at[hd], t).start()

    def norm_drain(hd):
        drain = ln_r.at[hd, pl.ds(0, chips - 1)]
        return remote(drain, drain, lx_s.at[hd], lx_r.at[hd], partner)

    send_hop = remote(dw_part, hop, misc_s.at[6], misc_r.at[6], partner)
    load_hop = pltpu.make_async_copy(hop, dw_part, load_sem.at[0])

    def dw_half(k):
        lanes = pl.ds(pl.multiple_of(k * half, half), half)
        return dot(own_hidden(0, nq, lanes), x_new[tok:2 * tok, :], 0, 0).reshape(SIDE, SIDE, blk, dim)

    def dw_begin():
        dw_part[...] = dw_half(1 - core)
        send_hop.start()
        d_x[extra % 3] = dw_half(core)
        dx_own[0:nq] = dot(x_new[tok:2 * tok, :], w2[...], 1, 1).reshape(nq, blk, dim)

    def dw_join():
        send_hop.wait()
        load_hop.start()
        load_hop.wait()
        d_x[extra % 3] = d_x[extra % 3] + dw_part[...]

    dw_mine = dw_out.at[core]
    save_dw = pltpu.make_async_copy(dw_own, dw_out.at[core, yy, xx], load_sem.at[1])
    send_dw = remote(dw_mine, dw_mine, misc_s.at[7], misc_r.at[7], partner)
    dw_other = dw_out.at[1 - core]

    def wg_copy(step, h, d, back=0):
        k = 0 if d == 1 else 1
        r = gathered(dw_mine, step, h, d, back)
        src = dw_own.at[:, cols_of(h)] if step == 0 and not back else r
        return remote(src, r, wg_s.at[step, h, k], wg_r.at[step, h, k], neighbour(h if step < 2 else 1 - h, d))

    def dw_gather(step):
        if step == 0:
            save_dw.start()
        else:
            for h in range(2):
                for d in DIRS:
                    wg_copy(step - 1, h, d, 1).wait_recv()
        if step == 2:
            save_dw.wait()
        if step == 4:
            send_dw.start()
            return
        for h in range(2):
            for d in DIRS:
                wg_copy(step, h, d).start()

    def give(h):
        lanes = slice(h * half, (h + 1) * half)
        return remote(d_e.at[other_rows, lanes], zt.at[pl.ds(h * rows, rows)], misc_s.at[3 + h], misc_r.at[3 + h], partner)

    m_v[...] = jnp.zeros(m_v.shape, F32)
    lse_v[...] = jnp.zeros(lse_v.shape, F32)
    remote(e_all.at[other_rows], e_all.at[other_rows], misc_s.at[1], misc_r.at[1], partner).wait()

    def item(s, carry):
        slot = lax.rem(s + 3, 3)
        is_dw = s == extra
        c = jnp.where(is_dw, -9, jnp.where(s < extra, s, s - 1))
        last = s == nch
        flow = (c >= -1) & (s < nch)
        pl.when(c >= 0)(lambda: stat_wait(c))
        pl.when(flow)(lambda: phase_one(c, 0, mid, True))
        pl.when(last)(lambda: phase_one(c, 0, mid, False))
        pl.when(is_dw)(lambda: norm_back(1))
        rs_step(1, 1, s - 1)
        pl.when(s == extra + 1)(lambda: rs_step(1, 0, extra))
        pl.when((s >= 0) & (s < nq))(lambda: ag_tick(2 * s + 6))
        pl.when(flow)(lambda: phase_one(c, mid, n_tiles, True))

        @pl.when(last)
        def _():
            phase_one(c, mid, n_tiles, False)
            pl.semaphore_signal(free_sem, inc=1, device_id=partner, device_id_type=MESH)
        pl.when(is_dw)(dw_begin)
        rs_step(3, 0, s - 2)
        pl.when(s == -1)(lambda: ag_tick(5))
        pl.when(s == extra + 4)(lambda: dw_gather(2))
        pl.when(c == -1)(lambda: exp_pass(c, slot, False))
        pl.when((c >= 0) & (s < nch))(lambda: exp_pass(c, slot, True))
        pl.when(last)(lambda: dx_half(slot, 0))
        pl.when(flow)(lambda: stat_send(c + 1))
        pl.when(is_dw)(dw_join)
        rs_step(0, 0, s)
        rs_step(3, 1, s - 2)
        pl.when((c >= -2) & (c < nq - 2))(lambda: ag_finish(c + 2))

        @pl.when((c >= 0) & (c < nq - 2))
        def _():
            project(lax.rem(c + 2, nq))
            dx_half(slot, 1)
        pl.when(c >= nq - 2)(lambda: dx_half(slot, 1))
        rs_step(0, 1, s)
        pl.when((s >= 0) & (s < nq))(lambda: ag_tick(2 * s + 7))
        pl.when(s == extra + 3)(lambda: dw_gather(0))
        three(c, False)

        @pl.when(last)
        def _():
            pl.semaphore_wait(free_sem, 1)
            for h in range(2):
                give(h).start()
        rs_step(2, 0, s - 1)
        rs_step(4, 0, s - 2)
        pl.when(s == extra + 4)(lambda: dw_gather(3))
        three(c, True)
        pl.when(s != extra)(lambda: rs_step(1, 0, s))
        rs_step(2, 1, s - 1)
        rs_step(4, 1, s - 2)
        pl.when(s == -2)(lambda: ag_tick(4))
        pl.when(s == extra + 3)(lambda: dw_gather(1))
        pl.when(s == extra + 5)(lambda: dw_gather(4))

        @pl.when(s != extra)
        def _():
            x_cur[...] = x_next[...]
            x_next[...] = x_new[...]
        return carry

    lax.fori_loop(-2, nch + 1, item, 0)

    s = nch
    send_l = remote(loss_v, loss_p, misc_s.at[5], misc_r.at[5], partner)
    send_l.start()
    rs_step(1, 1, s)
    rs_step(3, 0, s - 1)
    rs_step(3, 1, s - 1)
    for h in range(2):
        give(h).wait()
    outs = []
    out_tile = rows // 8
    for j in range(8):
        r = pl.ds(pl.multiple_of(core * rows + j * out_tile, 8), out_tile)
        for h in range(2):
            lanes = slice(h * half, (h + 1) * half)
            d_e[r, lanes] = d_e[r, lanes] + zt[h * rows + j * out_tile:h * rows + (j + 1) * out_tile, :]
        outs.append(pltpu.make_async_copy(d_e.at[r], de_out.at[pl.ds(j * out_tile, out_tile)], load_sem.at[2 + j]))
        outs[-1].start()
    rs_step(2, 0, s)
    rs_step(2, 1, s)
    rs_step(4, 0, s - 1)
    rs_step(4, 1, s - 1)
    rs_step(3, 0, s)
    rs_step(3, 1, s)
    send_l.wait()
    loss_out[core] = loss_v[...]
    loss_out[1 - core] = loss_p[...]
    cnt_out[...] = counts
    norm_drain(1).wait()
    for par in range(2):
        stat_drain(par).wait_send()
    for step in range(4):
        for h in range(2):
            for d in DIRS:
                wg_copy(step, h, d).wait_send()
    remote(dw_mine, dw_other, misc_s.at[7], misc_r.at[7], partner).wait()
    for o in outs:
        o.wait()
    rs_step(4, 0, s)
    rs_step(4, 1, s)
    norm_back(0)
    save_dh = pltpu.make_async_copy(x_new.at[pl.ds(0, tok)], dh_out, load_sem.at[0])
    save_dh.start()
    norm_drain(0).wait()
    for hd in range(2):
        ln_p[0, 2 * hd:2 * hd + 2, :] = jnp.sum(ln_r[hd], axis=0)
    swap = remote(ln_p.at[0], ln_p.at[1], misc_s.at[8], misc_r.at[8], partner)
    swap.start()
    swap.wait()
    ln_out[...] = ln_p[0] + ln_p[1]
    save_dh.wait()


def solution(mesh):
    tok_spec = P(('dp', 'tp'), None)
    row_spec = P(None, ('dp', 'tp'))
    chips = mesh.shape['tp'] // CORES
    assert math.isqrt(chips) == SIDE

    def run_kernel(info, hidden, w_two, gain, bias, embed):
        tok, dim = hidden.shape
        rows = embed.shape[0]
        blk = BLOCK
        nq = tok // blk
        nch, rpc, half, quart = 2 * nq, chips * blk, dim // 2, dim // 4
        vocab = CORES * rows
        vmem = pl.BlockSpec(memory_space=pltpu.VMEM)
        hbm = pl.BlockSpec(memory_space=pltpu.MemorySpace.HBM)
        dma = pltpu.SemaphoreType.DMA
        return pl.pallas_call(
            functools.partial(fused_kernel, nq),
            out_shape=(jax.ShapeDtypeStruct((tok, dim), BF16), jax.ShapeDtypeStruct((rows, dim), F32),
                       jax.ShapeDtypeStruct((CORES, SIDE, SIDE, blk, dim), F32),
                       jax.ShapeDtypeStruct((SIDE, SIDE, blk, dim), F32), jax.ShapeDtypeStruct((4, dim), F32),
                       jax.ShapeDtypeStruct((CORES, nch, 1, rpc), F32), jax.ShapeDtypeStruct((8, 128), F32)),
            in_specs=[vmem, hbm, hbm, vmem, vmem, hbm],
            out_specs=[hbm, hbm, hbm, hbm, vmem, vmem, vmem],
            scratch_shapes=[
                pltpu.VMEM((vocab, dim), BF16), pltpu.VMEM((vocab, dim), F32),
                pltpu.VMEM((vocab, rpc), F32), pltpu.VMEM((vocab, rpc), BF16),
                pltpu.VMEM((rpc, dim), BF16), pltpu.VMEM((rpc, dim), BF16), pltpu.VMEM((rpc, dim), BF16),
                pltpu.VMEM((nq, SIDE, SIDE, blk, dim), BF16), pltpu.VMEM((dim, dim), BF16),
                pltpu.VMEM((3, SIDE, SIDE, blk, dim), F32),
                pltpu.VMEM((3, 2, 2, SIDE, blk, quart), F32), pltpu.VMEM((3, 2, 2, SIDE, blk, half), F32),
                pltpu.VMEM((3, 2, 2, blk, quart), F32), pltpu.VMEM((3, 2, 2, blk, half), F32),
                pltpu.VMEM((chips, 8, tok), F32), pltpu.VMEM((nch, 1, rpc), jnp.int32),
                pltpu.VMEM((nch, 1, rpc), F32), pltpu.VMEM((nch, 1, rpc), F32), pltpu.VMEM((2, 8, 128), F32),
                pltpu.VMEM((2, 2, rpc), F32), pltpu.VMEM((2, chips, 2, rpc), F32),
                pltpu.VMEM((8, rpc), F32), pltpu.VMEM((1, rpc), F32), pltpu.VMEM((1, rpc), F32),
                pltpu.VMEM((1, rpc), F32), pltpu.VMEM((nch, 1, rpc), F32), pltpu.VMEM((nch, 1, rpc), F32),
                pltpu.VMEM((nch, blk, dim), F32),
                pltpu.VMEM((SIDE, SIDE, blk, dim), F32), pltpu.VMEM((blk, dim), F32),
                pltpu.VMEM((2, 2, dim), F32), pltpu.VMEM((2, chips, 2, dim), F32), pltpu.VMEM((2, 4, dim), F32),
                dma((2 + nq,)), dma((nq, 4, 2, 2)), dma((nq, 4, 2, 2)), dma((3, 4, 2, 2)), dma((3, 4, 2, 2)),
                dma((2,)), dma((2,)), dma((9,)), dma((9,)), dma((2,)), dma((2,)), dma((4, 2, 2)), dma((4, 2, 2)),
                pltpu.SemaphoreType.REGULAR,
            ],
            compiler_params=pltpu.CompilerParams(collective_id=0, has_side_effects=True,
                                                 vmem_limit_bytes=VMEM_BYTES),
            name='fused_heads',
        )(info, hidden, w_two, gain, bias, embed)

    def device_step(hidden, w_two, ln_scale, ln_shift, embed, targets, loss_mask):
        tok, dim = hidden.shape
        me = lax.axis_index('tp')
        info = jnp.concatenate([targets, loss_mask, jnp.zeros((4, tok), jnp.int32)]).astype(F32)
        d_hidden, d_embed, d_w_two, _, d_norm, losses, counts = run_kernel(info, hidden, w_two, ln_scale, ln_shift, embed)
        losses = losses.reshape(CORES, 2, -1, chips, BLOCK)[:, ::-1]
        mine = lax.dynamic_index_in_dim(losses, me % CORES, 0, keepdims=False)
        token_loss = lax.dynamic_index_in_dim(mine, me // CORES, 2, keepdims=False).reshape(2, tok)
        total_loss = jnp.sum(jnp.sum(losses, axis=(0, 2, 3, 4)) / counts[2:4, 0]).reshape(1)
        return token_loss, total_loss, d_hidden, d_embed, d_w_two.reshape(dim, dim), d_norm[0::2], d_norm[1::2]

    return jax.shard_map(device_step, mesh=mesh,
                         in_specs=(tok_spec, P(), P(), P(), P('tp', None), row_spec, row_spec),
                         out_specs=(row_spec, P('dp'), tok_spec, tok_spec, P('dp', None), P('dp', None), P('dp', None)),
                         check_vma=False)
```

```python
import functools
import math

import jax
import jax.numpy as jnp
from jax import lax
from jax.experimental import pallas as pl
from jax.experimental.pallas import tpu as pltpu
from jax.sharding import PartitionSpec as P

LN_EPS = 1e-5
BIG = 1e30
CORES = 2
SIDE = 4
BLOCK = 32
VMEM_BYTES = 67043328
F32 = jnp.float32
BF16 = jnp.bfloat16
MESH = pl.DeviceIdType.MESH
DIRS = (1, -1)


def guarded(cond, fn):
    if isinstance(cond, bool):
        if cond:
            fn()
    else:
        pl.when(cond)(fn)


def both(a, b):
    return a and b if isinstance(a, bool) else a & b


def layer_norm(values, gain, bias):
    mean_val = jnp.mean(values, axis=-1, keepdims=True)
    centered = values - mean_val
    variance = jnp.mean(centered * centered, axis=-1, keepdims=True)
    return centered * lax.rsqrt(variance + LN_EPS) * gain + bias


def dot(a, b, ca, cb):
    return lax.dot_general(a, b, (((ca,), (cb,)), ((), ())), preferred_element_type=F32)


def fused_kernel(nq, info_ref, hid_ref, w2_ref, gain_ref, bias_ref, emb_ref,
                 dh_out, de_out, dw_out, hop, dgain_out, dbias_out, loss_out, total_out,
                 e_all, d_e, zt, dzt, x_new, x_next, x_cur, h_all, w2, d_x, dw_part, r1, r2, r3, r4,
                 info_all, tgt_v, wgt_v, msk_v, cnt, stat_s, stat_r, m_v, lse_l, lse_v, shift_v, tgt_l, loss_v, loss_p,
                 dx_own, dw_own, ln_s, ln_r, ln_p,
                 load_sem, ag_s, ag_r, rs_s, rs_r, st_s, st_r, misc_s, misc_r, lx_s, lx_r, wg_s, wg_r, free_sem):
    nch = 2 * nq
    rows = emb_ref.shape[0]
    vocab = e_all.shape[0]
    dim = e_all.shape[1]
    half = dim // 2
    quart = dim // 4
    chips, blk = SIDE * SIDE, h_all.shape[3]
    tok = nq * blk
    turn = nq + 2
    rpc = chips * blk
    me = lax.axis_index('tp')
    core = lax.rem(me, CORES)
    chip = lax.div(me, CORES)
    yy = lax.div(chip, SIDE)
    xx = lax.rem(chip, SIDE)

    def wrap(v):
        return lax.rem(v + 2 * SIDE, SIDE)

    def dev(y, x, c):
        return {'tp': (y * SIDE + x) * CORES + c}

    partner = dev(yy, xx, 1 - core)
    peers = [dev(wrap(yy + dy), wrap(xx + dx), core) for dy in range(SIDE) for dx in range(SIDE) if dy or dx]

    def neighbour(axis, d):
        return dev(yy, wrap(xx + d), core) if axis == 0 else dev(wrap(yy + d), xx, core)

    def remote(src, dst, ssem, rsem, target):
        return pltpu.make_async_remote_copy(src_ref=src, dst_ref=dst, send_sem=ssem, recv_sem=rsem,
                                            device_id=target, device_id_type=MESH)

    my_rows = pl.ds(pl.multiple_of(core * rows, 128), rows)
    other_rows = pl.ds(pl.multiple_of((1 - core) * rows, 128), rows)
    load_e = pltpu.make_async_copy(emb_ref, e_all.at[my_rows], load_sem.at[0])
    load_w = pltpu.make_async_copy(w2_ref, w2, load_sem.at[1])
    load_h = [pltpu.make_async_copy(hid_ref.at[pl.ds(q * blk, blk)], h_all.at[q, yy, xx], load_sem.at[2 + q])
              for q in range(nq)]
    for c in load_h:
        c.start()
    load_e.start()
    load_w.start()

    barrier = pltpu.get_barrier_semaphore()
    for t in peers + [partner]:
        pl.semaphore_signal(barrier, inc=1, device_id=t, device_id_type=MESH)
    pl.semaphore_wait(barrier, len(peers) + 1)

    def coords(h):
        return (xx, yy) if h == 0 else (yy, xx)

    def sub(h, d):
        return pl.ds(h * half + (0 if d == 1 else quart), quart)

    def cols_of(h):
        return pl.ds(h * half, half)

    def gathered(buf, step, h, d, back):
        a, b = coords(h)
        if step == 0:
            pos, cols = (wrap(a - back * d), b), cols_of(h)
        elif step == 1:
            pos, cols = (wrap(a - (1 + back) * d), b), sub(h, d)
        elif step == 2:
            pos, cols = (None, wrap(b - back * d)), cols_of(h)
        else:
            pos, cols = (None, wrap(b - (1 + back) * d)), sub(h, d)
        px, py = pos if h == 0 else pos[::-1]
        py = slice(None) if py is None else py
        px = slice(None) if px is None else px
        return buf.at[py, px, :, cols]

    def ag_copy(step, h, q, d, back=0):
        k = 0 if d == 1 else 1
        r = gathered(h_all.at[q], step, h, d, back)
        return remote(r, r, ag_s.at[q, step, h, k], ag_r.at[q, step, h, k],
                      neighbour(h if step < 2 else 1 - h, d))

    def ag_start(step, q):
        for h in range(2):
            for d in DIRS:
                ag_copy(step, h, q, d).start()

    def ag_wait_recv(step, q):
        for h in range(2):
            for d in DIRS:
                ag_copy(step, h, q, d, 1).wait_recv()

    def ag_tick(k, steps=(3, 2, 1, 0)):
        for step in steps:
            q = k - step

            def go(step=step, q=q):
                if step > 0:
                    ag_wait_recv(step - 1, q)
                ag_start(step, q)
            guarded(both(q >= 0, q < nq), go)

    def ag_finish(q):
        ag_wait_recv(3, q)
        for step in range(4):
            for h in range(2):
                for d in DIRS:
                    ag_copy(step, h, q, d).wait_send()

    for c in load_h:
        c.wait()
    ag_tick(0)

    info_copies = [remote(info_ref, info_all.at[chip], misc_s.at[0], misc_r.at[0], t) for t in peers]
    for c in info_copies:
        c.start()
    info_all[chip] = info_ref[...]
    ag_tick(1)
    load_e.wait()
    send_e = remote(e_all.at[my_rows], e_all.at[my_rows], misc_s.at[1], misc_r.at[1], partner)
    send_e.start()
    ag_tick(2)
    every_info = info_all.at[pl.ds(0, chips - 1)]
    remote(every_info, every_info, misc_s.at[0], misc_r.at[0], partner).wait_recv()
    remote(every_info, every_info, misc_s.at[0], misc_r.at[0], partner).wait_send()
    total = jnp.zeros((8, rpc), F32)
    for q in range(nq):
        got = jnp.concatenate([info_all[o][:, q * blk:(q + 1) * blk] for o in range(chips)], axis=1)
        total = total + got
        for hd in range(2):
            c = (1 - hd) * nq + q
            tgt_v[c] = got[hd:hd + 1].astype(jnp.int32) - chip * vocab
            msk_v[c] = got[2 + hd:3 + hd]
    cnt[0] = jnp.broadcast_to(jnp.sum(total, axis=1, keepdims=True), cnt.shape[1:])
    send_c = remote(cnt.at[0], cnt.at[1], misc_s.at[2], misc_r.at[2], partner)
    send_c.start()
    ag_tick(3)
    send_c.wait()
    counts = cnt[0] + cnt[1]
    for hd in range(2):
        for q in range(nq):
            c = (1 - hd) * nq + q
            wgt_v[c] = msk_v[c] / counts[2 + hd:3 + hd, 0:1]
    load_w.wait()

    def part(buf, h, pos1, pos2, cols):
        px, py = (pos1, pos2) if h == 0 else (pos2, pos1)
        py = slice(None) if py is None else py
        px = slice(None) if px is None else px
        return buf.at[py, px, :, cols]

    def rs_run(step, h, buf, rslot, sslot, keep):
        a, b = coords(h)

        def copy(st, k):
            d = DIRS[k]
            if st == 0:
                src, dst = part(buf, h, wrap(a + 2), None, sub(h, d)), r1
            elif st == 1:
                src, dst = part(buf, h, wrap(a + d), None, cols_of(h)), r2
            elif st == 2:
                src, dst = part(buf, h, a, wrap(b + 2), sub(h, d)), r3
            else:
                src, dst = part(buf, h, a, wrap(b + d), cols_of(h)), r4
            return remote(src, dst.at[rslot, h, k], rs_s.at[sslot, st, h, k], rs_r.at[rslot, st, h, k],
                          neighbour(h if st < 2 else 1 - h, d))

        if step > 0:
            for k in range(2):
                copy(step - 1, k).wait_recv()
        if step == 1:
            for k, d in enumerate(DIRS):
                r = part(buf, h, wrap(a + d), None, sub(h, d))
                r[...] = r[...] + r1[rslot, h, k]
        elif step == 2:
            r = part(buf, h, a, None, cols_of(h))
            r[...] = r[...] + r2[rslot, h, 0] + r2[rslot, h, 1]
        elif step == 3:
            for k, d in enumerate(DIRS):
                r = part(buf, h, a, wrap(b + d), sub(h, d))
                r[...] = r[...] + r3[rslot, h, k]
        elif step == 4:
            keep(part(buf, h, a, b, cols_of(h))[...] + r4[rslot, h, 0] + r4[rslot, h, 1])
        if step < 4:
            for k in range(2):
                copy(step, k).start()
        else:
            for st in range(4):
                for k in range(2):
                    copy(st, k).wait_send()

    def rs_step(step, h, c):
        rem = (lambda v, n: v % n) if isinstance(c, int) else (lambda v, n: lax.rem(v + 12, n))
        slot = rem(c, 3)

        def keep(val):
            dx_own[c, :, h * half:(h + 1) * half] = val
        guarded(both(c >= 0, c < nch), lambda: rs_run(step, h, d_x.at[slot], rem(c, 2), slot, keep))

    def rs_dw(step):
        for h in range(2):
            def keep(val, h=h):
                dw_own[:, h * half:(h + 1) * half] = val
            rs_run(step, h, dw_part, 2, 3, keep)

    def stat_drain(par):
        drain = stat_r.at[par, pl.ds(0, chips - 1)]
        return remote(drain, drain, st_s.at[par], st_r.at[par], partner)

    def stat_send(e):
        par = lax.rem(e, 2)
        pl.when(e >= 2)(lambda: stat_drain(par).wait_send())
        stat_s[par, 0:1, :] = lse_l[...]
        stat_s[par, 1:2, :] = tgt_l[...]
        stat_r[par, chip] = stat_s[par]
        for t in peers:
            remote(stat_s.at[par], stat_r.at[par, chip], st_s.at[par], st_r.at[par], t).start()

    def stat_wait(e):
        par = e % 2 if isinstance(e, int) else lax.rem(e, 2)
        stat_drain(par).wait_recv()
        got = stat_r[par]

        def put():
            loss_v[e - 1] = (lse_v[...] - jnp.sum(got[:, 1, :], axis=0, keepdims=True)) * msk_v[e - 1]
        guarded(e >= 1, put)
        if isinstance(e, int):
            return
        lse = got[:, 0, :]
        top = jnp.max(lse, axis=0, keepdims=True)
        lse = top + jnp.log(jnp.sum(jnp.exp(lse - top), axis=0, keepdims=True))
        lse_v[...] = lse
        wgt = wgt_v[e]
        live = wgt > 0.0
        shift_v[...] = jnp.where(live, lse - jnp.log(jnp.where(live, wgt, 1.0)), BIG)

    tile = 256

    def project(q):
        h = h_all[q].reshape(rpc, dim)
        for n0 in range(0, dim, half):
            x_new[:, n0:n0 + half] = dot(h, w2[:, n0:n0 + half], 1, 0).astype(BF16)

    def fetch(c):
        q = lax.rem(c, nq)
        pl.when(c < nq)(lambda: project(q))

        @pl.when(c >= nq)
        def _():
            x_new[...] = h_all[q].reshape(rpc, dim)

    def norm_rows(hd, lo, hi):
        step = 64
        gain, bias = gain_ref[pl.ds(hd, 1), :], bias_ref[pl.ds(hd, 1), :]
        for r in range(lo, hi, step):
            x_new[r:r + step, :] = layer_norm(x_new[r:r + step, :].astype(F32), gain, bias).astype(BF16)

    def logits_tile(v0, top):
        z = dot(e_all[v0:v0 + tile, :], x_next[...], 1, 1)
        zt[v0:v0 + tile, :] = z
        return jnp.maximum(top, jnp.max(z.reshape(tile // 8, 8, rpc), axis=0))

    def strips(c):
        tgt = tgt_v[c]
        return jnp.where(lax.broadcasted_iota(jnp.int32, (8, rpc), 0) == (tgt & 7), tgt >> 3, -1)

    def grad_tile(v0, shift, where8, wgt):
        prob = jnp.exp(zt[v0:v0 + tile, :] - shift).reshape(tile // 8, 8, rpc)
        hit = lax.broadcasted_iota(jnp.int32, (tile // 8, 8, rpc), 0) == (where8 - v0 // 8)[None]
        dzt[v0:v0 + tile, :] = jnp.where(hit, prob - wgt[None], prob).reshape(tile, rpc).astype(BF16)

    n_tiles = vocab // tile

    def phase_one(c, with_logits):
        at = jnp.maximum(c, 0)
        shift, where8, wgt = shift_v[...], strips(at), wgt_v[at]
        top = jnp.full((8, rpc), -jnp.inf, F32)
        for j in range(n_tiles):
            grad_tile(j * tile, shift, where8, wgt)
            if with_logits:
                top = logits_tile(j * tile, top)
        if with_logits:
            m_v[...] = top

    def dx_half(slot, h):
        val = dot(dzt[...], e_all[:, h * half:(h + 1) * half], 0, 0)
        d_x[slot, :, :, :, h * half:(h + 1) * half] = val.reshape(SIDE, SIDE, blk, half)

    def exp_pass(slot=None):
        top = jnp.max(m_v[...], axis=0, keepdims=True)
        acc = jnp.zeros((8, rpc), F32)
        for j in range(n_tiles):
            prob = jnp.exp(zt[j * tile:(j + 1) * tile, :] - top)
            acc = acc + jnp.sum(prob.reshape(tile // 8, 8, rpc), axis=0)
        if slot is not None:
            dx_half(slot, 0)
        lse_l[...] = top + jnp.log(jnp.sum(acc, axis=0, keepdims=True))

    de_tile = rows // 4

    def phase_three(c, with_grad, norm):
        hd = jnp.where(c + 2 < nq, 1, 0)
        where8 = strips(jnp.clip(c + 1, 0, nch - 1))
        found = jnp.zeros((8, rpc), F32)
        if with_grad and norm:
            dx_half(lax.rem(c + 3, 3), 1)
        for j in range(8):
            base = (core if j >= 4 else 1 - core) * rows
            if norm:
                norm_rows(hd, j * rpc // 8, (j + 1) * rpc // 8)
                for v0 in range(j * de_tile, (j + 1) * de_tile, 8):
                    found = jnp.where(where8 == v0 // 8, zt[v0:v0 + 8, :], found)
            if with_grad:
                r = pl.ds(pl.multiple_of(base + j % 4 * de_tile, 32), de_tile)
                d_e[r, :] = d_e[r, :] + dot(dzt[r, :], x_cur[...], 1, 0)
        tgt_l[...] = jnp.sum(found, axis=0, keepdims=True)

    def own_hidden(j, n, lanes=slice(None)):
        return h_all[j:j + n, yy, xx, :, lanes].reshape(n * blk, -1)

    def norm_back(hd, lo=0, hi=nq // 2):
        step = 2 * blk
        d_gain = jnp.zeros((8, dim), F32)
        d_bias = jnp.zeros((8, dim), F32)
        if hd == 1:
            for n0 in range(0, dim, half):
                x_new[0:tok, n0:n0 + half] = dot(own_hidden(0, nq), w2[:, n0:n0 + half], 1, 0).astype(BF16)
        for j in range(lo, hi):
            r = j * step
            val = (x_new[r:r + step, :] if hd == 1 else own_hidden(2 * j, 2)).astype(F32)
            cen = val - jnp.mean(val, axis=-1, keepdims=True)
            rstd = lax.rsqrt(jnp.mean(cen * cen, axis=-1, keepdims=True) + LN_EPS)
            hat = cen * rstd
            at = (1 - hd) * nq + 2 * j
            d_y = dx_own[at:at + 2].reshape(step, dim)
            d_gain = d_gain + jnp.sum((d_y * hat).reshape(step // 8, 8, dim), axis=0)
            d_bias = d_bias + jnp.sum(d_y.reshape(step // 8, 8, dim), axis=0)
            g = d_y * gain_ref[hd:hd + 1, :]
            d_in = rstd * (g - jnp.mean(g, axis=-1, keepdims=True) - hat * jnp.mean(g * hat, axis=-1, keepdims=True))
            if hd == 1:
                x_new[tok + r:tok + r + step, :] = d_in.astype(BF16)
            else:
                x_new[r:r + step, :] = (d_in + dx_own[2 * j:2 * j + 2].reshape(step, dim)).astype(BF16)
        sums = (jnp.sum(d_gain, axis=0, keepdims=True), jnp.sum(d_bias, axis=0, keepdims=True))
        for k in range(2):
            ln_s[hd, k:k + 1, :] = sums[k] if lo == 0 else ln_s[hd, k:k + 1, :] + sums[k]
        if hi < nq // 2:
            return
        ln_r[hd, chip] = ln_s[hd]
        for t in peers:
            remote(ln_s.at[hd], ln_r.at[hd, chip], lx_s.at[hd], lx_r.at[hd], t).start()

    def norm_drain(hd):
        drain = ln_r.at[hd, pl.ds(0, chips - 1)]
        return remote(drain, drain, lx_s.at[hd], lx_r.at[hd], partner)

    dw_half_rows = SIDE // 2

    def dw_rows(k, p):
        lanes = pl.ds(pl.multiple_of(k * half + p * quart, quart), quart)
        return dot(own_hidden(0, nq, lanes), x_new[tok:2 * tok, :], 0, 0)

    def send_hop(p):
        stage = dx_own.at[pl.ds((1 - p) * nq, nq)]
        return remote(stage, hop.at[p], misc_s.at[6 + p], misc_r.at[6 + p], partner)

    def load_hop(p):
        return pltpu.make_async_copy(hop.at[p], dx_own.at[pl.ds(nq, nq)], load_sem.at[0])

    def dw_begin():
        norm_back(1)
        for p in range(2):
            dx_own[(1 - p) * nq:(2 - p) * nq] = dw_rows(1 - core, p).reshape(nq, blk, dim)
            send_hop(p).start()
        for p in range(2):
            dw_part[p * dw_half_rows:(p + 1) * dw_half_rows] = dw_rows(core, p).reshape(dw_half_rows, SIDE, blk, dim)

    def dw_mid():
        for p in range(2):
            send_hop(p).wait()
        load_hop(0).start()
        dx_own[0:nq] = dot(x_new[tok:2 * tok, :], w2[...], 1, 1).reshape(nq, blk, dim)

    def dw_add(p):
        load_hop(p).wait()
        r = dw_part.at[pl.ds(p * dw_half_rows, dw_half_rows)]
        r[...] = r[...] + dx_own[nq:2 * nq].reshape(dw_half_rows, SIDE, blk, dim)
        if p == 0:
            load_hop(1).start()
        else:
            rs_dw(0)

    dw_mine = dw_out.at[core]
    save_dw = pltpu.make_async_copy(dw_own, dw_out.at[core, yy, xx], load_sem.at[1])
    send_dw = remote(dw_mine, dw_mine, misc_s.at[9], misc_r.at[9], partner)
    dw_other = dw_out.at[1 - core]

    def wg_copy(step, h, d, back=0):
        k = 0 if d == 1 else 1
        r = gathered(dw_mine, step, h, d, back)
        src = dw_own.at[:, cols_of(h)] if step == 0 and not back else r
        return remote(src, r, wg_s.at[step, h, k], wg_r.at[step, h, k], neighbour(h if step < 2 else 1 - h, d))

    def dw_gather(step):
        if step == 0:
            save_dw.start()
        else:
            for h in range(2):
                for d in DIRS:
                    wg_copy(step - 1, h, d, 1).wait_recv()
        if step == 2:
            save_dw.wait()
        if step == 4:
            send_dw.start()
            return
        for h in range(2):
            for d in DIRS:
                wg_copy(step, h, d).start()

    def give(h):
        lanes = slice(h * half, (h + 1) * half)
        return remote(d_e.at[other_rows, lanes], zt.at[pl.ds(h * rows, rows)], misc_s.at[3 + h], misc_r.at[3 + h], partner)

    m_v[...] = jnp.zeros(m_v.shape, F32)
    lse_v[...] = jnp.zeros(lse_v.shape, F32)
    lse_l[...] = jnp.zeros(lse_l.shape, F32)
    shift_v[...] = jnp.zeros(shift_v.shape, F32)
    remote(e_all.at[other_rows], e_all.at[other_rows], misc_s.at[1], misc_r.at[1], partner).wait()

    def chunk(i, carry):
        c = i - 2
        slot = lax.rem(i + 1, 3)
        last = c == nch - 1
        flow = (c >= -1) & (c < nch - 1)

        def at(k, fn):
            pl.when(c == k)(fn)

        pl.when(c >= 0)(lambda: stat_wait(c))
        pl.when(flow)(lambda: phase_one(c, True))
        rs_step(4, 1, c - 3)

        @pl.when(last)
        def _():
            phase_one(c, False)
            dx_half(slot, 0)
            dx_half(slot, 1)
        rs_step(2, 1, c - 2)
        rs_step(3, 0, c - 2)
        rs_step(1, 0, c - 1)
        at(turn, dw_begin)
        at(turn + 3, lambda: rs_dw(3))
        at(0, lambda: ag_tick(6))
        at(-1, exp_pass)

        @pl.when((c >= 0) & (c < nch - 1))
        def _():
            exp_pass(slot)
        pl.when(c >= -1)(lambda: stat_send(c + 1))
        rs_step(0, 0, c)
        pl.when(last)(lambda: rs_step(0, 1, c))
        rs_step(1, 1, c - 1)
        at(turn, dw_mid)
        at(turn + 1, lambda: rs_dw(1))
        at(turn + 4, lambda: dw_gather(1))
        at(-1, lambda: ag_tick(5))
        pl.when(c < nq - 2)(lambda: ag_finish(c + 2))
        pl.when(c < nch - 2)(lambda: fetch(c + 2))
        pl.when(c < 0)(lambda: phase_three(c, False, True))
        pl.when((c >= 0) & (c < nch - 1))(lambda: phase_three(c, True, True))
        pl.when(last)(lambda: phase_three(c, True, False))

        @pl.when(c == -1)
        def _():
            d_e[...] = jnp.zeros(d_e.shape, F32)

        @pl.when(last)
        def _():
            rs_step(1, 0, c)
            rs_step(1, 1, c)
        rs_step(2, 0, c - 1)
        pl.when(c < nch - 1)(lambda: rs_step(0, 1, c))

        @pl.when(c == turn)
        def _():
            dw_add(0)
            dw_add(1)
        rs_step(3, 1, c - 2)
        rs_step(4, 0, c - 2)
        at(turn + 2, lambda: rs_dw(2))

        @pl.when(c == turn + 3)
        def _():
            rs_dw(4)
            dw_gather(0)
        at(turn + 4, lambda: dw_gather(2))
        pl.when((c >= 1) & (c <= 3))(lambda: ag_tick(c + 7, (3, 2, 1)))
        at(-2, lambda: ag_tick(4))
        at(0, lambda: ag_tick(7))
        x_cur[...] = x_next[...]
        x_next[...] = x_new[...]
        return carry

    lax.fori_loop(0, nch + 2, chunk, 0)

    c = nch - 1
    pl.semaphore_signal(free_sem, inc=1, device_id=partner, device_id_type=MESH)
    dw_gather(3)
    stat_wait(nch)
    send_l = remote(loss_v, loss_p, misc_s.at[5], misc_r.at[5], partner)
    send_l.start()
    pl.semaphore_wait(free_sem, 1)
    for h in range(2):
        give(h).start()
    rs_step(4, 1, c - 2)
    rs_step(2, 1, c - 1)
    rs_step(3, 0, c - 1)
    rs_step(2, 0, c)
    rs_step(2, 1, c)
    rs_step(3, 1, c - 1)
    rs_step(4, 0, c - 1)
    rs_step(3, 0, c)
    rs_step(3, 1, c)
    rs_step(4, 1, c - 1)
    dw_gather(4)
    for h in range(2):
        give(h).wait()
    outs = []
    out_tile = rows // 8
    for j in range(8):
        r = pl.ds(pl.multiple_of(core * rows + j * out_tile, 8), out_tile)
        for h in range(2):
            lanes = slice(h * half, (h + 1) * half)
            d_e[r, lanes] = d_e[r, lanes] + zt[h * rows + j * out_tile:h * rows + (j + 1) * out_tile, :]
        outs.append(pltpu.make_async_copy(d_e.at[r], de_out.at[pl.ds(j * out_tile, out_tile)], load_sem.at[2 + j]))
        outs[-1].start()
    send_l.wait()
    mine = jnp.concatenate([loss_v[k] for k in range(nch)], axis=0)
    every = jnp.sum(mine + jnp.concatenate([loss_p[k] for k in range(nch)], axis=0), axis=1, keepdims=True)
    total_out[...] = sum(jnp.sum(every[(1 - hd) * nq:(2 - hd) * nq], axis=0, keepdims=True) / counts[2 + hd:3 + hd, 0:1]
                         for hd in range(2))
    own = mine[:, 0:blk]
    for o in range(1, chips):
        own = jnp.where(chip == o, mine[:, o * blk:(o + 1) * blk], own)
    for hd in range(2):
        k = (1 - hd) * nq
        loss_out[hd:hd + 1, :] = jnp.concatenate([own[k + q:k + q + 1] for q in range(nq)], axis=1)
    norm_drain(1).wait()
    for par in range(2):
        stat_drain(par).wait_send()
    for step in range(4):
        for h in range(2):
            for d in DIRS:
                wg_copy(step, h, d).wait_send()
    remote(dw_mine, dw_other, misc_s.at[9], misc_r.at[9], partner).wait()
    for o in outs:
        o.wait()
    norm_back(0, 0, nq // 2 - 1)
    rs_step(4, 0, c)
    rs_step(4, 1, c)
    norm_back(0, nq // 2 - 1)
    save_dh = pltpu.make_async_copy(x_new.at[pl.ds(0, tok)], dh_out, load_sem.at[0])
    save_dh.start()
    norm_drain(0).wait()
    for hd in range(2):
        ln_p[0, 2 * hd:2 * hd + 2, :] = jnp.sum(ln_r[hd], axis=0)
    swap = remote(ln_p.at[0], ln_p.at[1], misc_s.at[8], misc_r.at[8], partner)
    swap.start()
    swap.wait()
    for hd in range(2):
        k = 2 * hd
        dgain_out[hd:hd + 1, :] = ln_p[0, k:k + 1, :] + ln_p[1, k:k + 1, :]
        dbias_out[hd:hd + 1, :] = ln_p[0, k + 1:k + 2, :] + ln_p[1, k + 1:k + 2, :]
    save_dh.wait()


def copy_kernel(de_in, dw_in, dh_in, a_in, b_in, c_in, d_in, de_out, dw_out, dh_out, a_out, b_out, c_out, d_out,
                de_v, dw_v, dh_v, in_sem, out_sem):
    jobs = []
    for src, buf, dst, tiles in ((de_in, de_v, de_out, 8), (dw_in, dw_v, dw_out, 4), (dh_in, dh_v, dh_out, 1)):
        n = src.shape[0] // tiles
        jobs += [(src.at[pl.ds(j * n, n)], buf.at[pl.ds(j * n, n)], dst.at[pl.ds(j * n, n)]) for j in range(tiles)]
    loads = [pltpu.make_async_copy(src, buf, in_sem.at[j]) for j, (src, buf, _) in enumerate(jobs)]
    saves = [pltpu.make_async_copy(buf, dst, out_sem.at[j]) for j, (_, buf, dst) in enumerate(jobs)]
    for c in loads:
        c.start()
    for src, dst in ((a_in, a_out), (b_in, b_out), (c_in, c_out), (d_in, d_out)):
        dst[...] = src[...]
    for load, save in zip(loads, saves):
        load.wait()
        save.start()
    for c in saves:
        c.wait()


def solution(mesh):
    tok_spec = P(('dp', 'tp'), None)
    row_spec = P(None, ('dp', 'tp'))
    chips = mesh.shape['tp'] // CORES
    assert math.isqrt(chips) == SIDE

    def run_kernel(info, hidden, w_two, gain, bias, embed):
        tok, dim = hidden.shape
        rows = embed.shape[0]
        blk = BLOCK
        nq = tok // blk
        nch, rpc, half, quart = 2 * nq, chips * blk, dim // 2, dim // 4
        vocab = CORES * rows
        vmem = pl.BlockSpec(memory_space=pltpu.VMEM)
        hbm = pl.BlockSpec(memory_space=pltpu.MemorySpace.HBM)
        dma = pltpu.SemaphoreType.DMA
        return pl.pallas_call(
            functools.partial(fused_kernel, nq),
            out_shape=(jax.ShapeDtypeStruct((tok, dim), BF16), jax.ShapeDtypeStruct((rows, dim), F32),
                       jax.ShapeDtypeStruct((CORES, SIDE, SIDE, blk, dim), F32),
                       jax.ShapeDtypeStruct((2, nq, blk, dim), F32), jax.ShapeDtypeStruct((2, dim), F32),
                       jax.ShapeDtypeStruct((2, dim), F32), jax.ShapeDtypeStruct((2, tok), F32),
                       jax.ShapeDtypeStruct((1, 1), F32)),
            in_specs=[vmem, hbm, hbm, vmem, vmem, hbm],
            out_specs=[hbm, hbm, hbm, hbm, vmem, vmem, vmem, vmem],
            scratch_shapes=[
                pltpu.VMEM((vocab, dim), BF16), pltpu.VMEM((vocab, dim), F32),
                pltpu.VMEM((vocab, rpc), F32), pltpu.VMEM((vocab, rpc), BF16),
                pltpu.VMEM((rpc, dim), BF16), pltpu.VMEM((rpc, dim), BF16), pltpu.VMEM((rpc, dim), BF16),
                pltpu.VMEM((nq, SIDE, SIDE, blk, dim), BF16), pltpu.VMEM((dim, dim), BF16),
                pltpu.VMEM((3, SIDE, SIDE, blk, dim), F32), pltpu.VMEM((SIDE, SIDE, blk, dim), F32),
                pltpu.VMEM((3, 2, 2, SIDE, blk, quart), F32), pltpu.VMEM((3, 2, 2, SIDE, blk, half), F32),
                pltpu.VMEM((3, 2, 2, blk, quart), F32), pltpu.VMEM((3, 2, 2, blk, half), F32),
                pltpu.VMEM((chips, 8, tok), F32), pltpu.VMEM((nch, 1, rpc), jnp.int32),
                pltpu.VMEM((nch, 1, rpc), F32), pltpu.VMEM((nch, 1, rpc), F32), pltpu.VMEM((2, 8, 128), F32),
                pltpu.VMEM((2, 2, rpc), F32), pltpu.VMEM((2, chips, 2, rpc), F32),
                pltpu.VMEM((8, rpc), F32), pltpu.VMEM((1, rpc), F32), pltpu.VMEM((1, rpc), F32),
                pltpu.VMEM((1, rpc), F32), pltpu.VMEM((1, rpc), F32),
                pltpu.VMEM((nch, 1, rpc), F32), pltpu.VMEM((nch, 1, rpc), F32),
                pltpu.VMEM((nch, blk, dim), F32),
                pltpu.VMEM((blk, dim), F32),
                pltpu.VMEM((2, 2, dim), F32), pltpu.VMEM((2, chips, 2, dim), F32), pltpu.VMEM((2, 4, dim), F32),
                dma((2 + nq,)), dma((nq, 4, 2, 2)), dma((nq, 4, 2, 2)), dma((4, 4, 2, 2)), dma((3, 4, 2, 2)),
                dma((2,)), dma((2,)), dma((10,)), dma((10,)), dma((2,)), dma((2,)), dma((4, 2, 2)), dma((4, 2, 2)),
                pltpu.SemaphoreType.REGULAR,
            ],
            compiler_params=pltpu.CompilerParams(collective_id=0, has_side_effects=True,
                                                 vmem_limit_bytes=VMEM_BYTES),
            name='fused_heads',
        )(info, hidden, w_two, gain, bias, embed)

    def device_step(hidden, w_two, ln_scale, ln_shift, embed, targets, loss_mask):
        tok, dim = hidden.shape
        info = jnp.concatenate([targets, loss_mask, jnp.zeros((4, tok), jnp.int32)]).astype(F32)
        d_hidden, d_embed, d_w_two, _, d_scale, d_shift, token_loss, total_loss = run_kernel(
            info, hidden, w_two, ln_scale, ln_shift, embed)
        d_w_two = d_w_two.reshape(dim, dim)
        arrays = (d_embed, d_w_two, d_hidden, d_scale, d_shift, token_loss, total_loss)
        specs = [pl.BlockSpec(memory_space=pltpu.MemorySpace.HBM)] * 3 + [pl.BlockSpec(memory_space=pltpu.VMEM)] * 4
        d_embed, d_w_two, d_hidden, d_scale, d_shift, token_loss, total_loss = pl.pallas_call(
            copy_kernel, out_shape=tuple(jax.ShapeDtypeStruct(v.shape, v.dtype) for v in arrays),
            in_specs=specs, out_specs=specs,
            scratch_shapes=[pltpu.VMEM(v.shape, v.dtype) for v in arrays[:3]] + [pltpu.SemaphoreType.DMA((13,))] * 2,
            compiler_params=pltpu.CompilerParams(vmem_limit_bytes=VMEM_BYTES), name='store_results',
        )(*arrays)
        return (token_loss, total_loss.reshape(1), d_hidden, d_embed, d_w_two, d_scale, d_shift)

    return jax.shard_map(device_step, mesh=mesh,
                         in_specs=(tok_spec, P(), P(), P(), P('tp', None), row_spec, row_spec),
                         out_specs=(row_spec, P('dp'), tok_spec, tok_spec, P('dp', None), P('dp', None), P('dp', None)),
                         check_vma=False)
```
